8 devices in a mesh: data: 2 (over z, y), time: 4 (over x, core).
Axes of the slice: x: 2, y: 2, z: 1, core: 2. Of those that a mesh axis runs over, the one named last changes fastest.
Arguments:
- x_init: float32 [32, 256, 768], P('data'), parts along dimension 0
- w_in: bfloat16 [768, 3072], replicated
- w_out: bfloat16 [3072, 768], replicated
- mod_gamma: bfloat16 [16, 3072], P('time')
- mod_beta: bfloat16 [16, 3072], P('time')
- step_size: float32 [16], P('time')
Outputs:
- output: float32 [32, 256, 768], P('data'), parts along dimension 0
There are 2 independent parts. The reference program is written for one: setup_inputs(seed, part) draws one part's arguments, and reference() takes and returns one part's arrays. A program takes and returns all parts, laid end to end along the dimension named above; an argument that names none is the same for every part.
All inputs are finite; a program needn't handle non-finite values.
Results may differ from the reference program's by a relative error of at most 0.0018853.
Values are sent between devices in bfloat16 or wider.
A program may use at most 1 GiB of HBM per device.

```python
import jax
import jax.numpy as jnp
from jax import lax

SAMPLES = 16
TOKENS = 256
CHANNELS = 768
HIDDEN = 3072
NUM_STEPS = 16
SWEEPS = 4


def setup_inputs(seed: int = 0, part: int = 0) -> dict:
    base_key = jax.random.key(seed)
    part_key = jax.random.fold_in(base_key, part)
    sub_keys = jax.random.split(base_key, 6)
    x_init = jax.random.normal(part_key, (SAMPLES, TOKENS, CHANNELS), jnp.float32)
    w_in = (jax.random.normal(sub_keys[0], (CHANNELS, HIDDEN), jnp.float32) * CHANNELS ** -0.5).astype(jnp.bfloat16)
    w_out = (jax.random.normal(sub_keys[1], (HIDDEN, CHANNELS), jnp.float32) * HIDDEN ** -0.5).astype(jnp.bfloat16)
    mod_gamma = (0.5 * jax.random.normal(sub_keys[2], (NUM_STEPS, HIDDEN), jnp.float32)).astype(jnp.bfloat16)
    mod_beta = jax.random.normal(sub_keys[3], (NUM_STEPS, HIDDEN), jnp.float32).astype(jnp.bfloat16)
    total_time = 1.0 + 2.0 * jax.random.uniform(sub_keys[4], (), jnp.float32)
    step_size = (0.5 + jax.random.uniform(sub_keys[5], (NUM_STEPS,), jnp.float32)) * (total_time / NUM_STEPS)
    return {"x_init": x_init, "w_in": w_in, "w_out": w_out, "mod_gamma": mod_gamma, "mod_beta": mod_beta, "step_size": step_size}


def drift_of(latents, w_in, w_out, gamma_j, beta_j, h_step):
    pre_act = jnp.dot(latents.astype(jnp.bfloat16).reshape(-1, CHANNELS), w_in, preferred_element_type=jnp.float32)
    hidden_act = jax.nn.gelu(pre_act * (1.0 + gamma_j.astype(jnp.float32)) + beta_j.astype(jnp.float32), approximate=True).astype(jnp.bfloat16)
    proj_out = jnp.dot(hidden_act, w_out, preferred_element_type=jnp.float32)
    return h_step * proj_out.reshape(latents.shape)


def reference(x_init, w_in, w_out, mod_gamma, mod_beta, step_size):
    run_init = jnp.zeros((SWEEPS,) + x_init.shape, jnp.float32)

    def step_body(run_sums, step_in):
        gamma_j, beta_j, h_step = step_in
        latents = jnp.concatenate([x_init[None], x_init[None] + run_sums[:-1]], axis=0)
        return run_sums + drift_of(latents, w_in, w_out, gamma_j, beta_j, h_step), None

    run_sums, _ = lax.scan(step_body, run_init, (mod_gamma, mod_beta, step_size))
    return x_init + run_sums[-1]
```

```python
import jax
import jax.numpy as jnp
from jax import lax
from jax.experimental import pallas as pl
from jax.experimental.pallas import tpu as pltpu
from jax.sharding import PartitionSpec as P

R = 256
C = 768
D = 3072
T = 16
NB = D // 256
K2 = 2.0 * 0.7978845608028654
K3 = 8.0 * 0.7978845608028654 * 0.044715

def gelu_mod(a, g, b):
    u = a * g + b
    p = (u * u) * K3 + K2
    t = jnp.tanh(u * p)
    return (u * t + u).astype(jnp.bfloat16)

def kernel(t_ref, x_ref, win_ref, wout_ref, g_ref, b_ref, h_ref, hs_ref, o_ref, a0, lat, latb, hid, s_acc):
    xb = x_ref[...].astype(jnp.bfloat16)
    for n in range(NB):
        a0[:, n * 256:(n + 1) * 256] = jnp.dot(xb, win_ref[:, n * 256:(n + 1) * 256], preferred_element_type=jnp.float32)
    s_acc[...] = jnp.zeros_like(s_acc)

    def step(j, lo, hi, fresh):
        lo1 = max(lo, 1)
        r0, r1 = (lo1 - 1) * R, hi * R
        for n in range(NB):
            cs = slice(n * 256, (n + 1) * 256)
            g = g_ref[pl.ds(j, 1), cs]
            b = b_ref[pl.ds(j, 1), cs]
            if lo == 0:
                hid[0:R, cs] = gelu_mod(a0[:, cs], g, b)
            if hi >= 1:
                a = jnp.dot(latb[r0:r1, :], win_ref[:, cs], preferred_element_type=jnp.float32)
                hv = gelu_mod(a, g, b)
                for s in range(lo1, hi + 1):
                    part = hv[(s - lo1) * R:(s - lo1 + 1) * R]
                    if s <= 2:
                        hid[s * R:(s + 1) * R, cs] = part
                    else:
                        s_acc[:, cs] += part.astype(jnp.float32) * hs_ref[pl.ds(j, 1), cs]
        hi2 = min(hi, 2)
        if lo <= hi2:
            for m in range(3):
                ms = slice(m * 256, (m + 1) * 256)
                d = jnp.dot(hid[lo * R:(hi2 + 1) * R, :], wout_ref[:, ms], preferred_element_type=jnp.float32)
                d = d * h_ref[pl.ds(j, 1), ms]
                for s in reversed(range(lo, hi2 + 1)):
                    rs = slice(s * R, (s + 1) * R)
                    if s == fresh:
                        base = x_ref[:, ms] if s == 0 else lat[(s - 1) * R:s * R, ms]
                    else:
                        base = lat[rs, ms]
                    new = base + d[(s - lo) * R:(s - lo + 1) * R]
                    lat[rs, ms] = new
                    latb[rs, ms] = new.astype(jnp.bfloat16)

    step(0, 0, 0, 0)
    step(1, 0, 1, 1)
    step(2, 0, 2, 2)
    o_ref[...] = lat[2 * R:3 * R, :]
    @pl.loop(3, 13)
    def _(j):
        step(j, 0, 3, -1)
    step(13, 1, 3, -1)
    step(14, 2, 3, -1)
    step(15, 3, 3, -1)
    for n in range(NB):
        cs = slice(n * 256, (n + 1) * 256)
        sv = s_acc[:, cs]
        hi_ = sv.astype(jnp.bfloat16)
        r = sv - hi_.astype(jnp.float32)
        mid = r.astype(jnp.bfloat16)
        hid[0:R, cs] = hi_
        hid[R:2 * R, cs] = mid
        hid[2 * R:3 * R, cs] = (r - mid.astype(jnp.float32)).astype(jnp.bfloat16)
    for m in range(3):
        ms = slice(m * 256, (m + 1) * 256)
        d = jnp.dot(hid[...], wout_ref[:, ms], preferred_element_type=jnp.float32)
        o_ref[:, ms] = o_ref[:, ms] + (d[0:R] + (d[R:2 * R] + d[2 * R:3 * R])) * h_ref[T:T + 1, ms]


def solution(mesh):
    groups = mesh.shape["time"]

    def local_run(x_init, w_in, w_out, mod_gamma, mod_beta, step_size):
        samples, tokens, _ = x_init.shape
        rows = samples * tokens // groups
        me = lax.axis_index("time")
        gamma = lax.all_gather(mod_gamma, "time", tiled=True).astype(jnp.float32)
        beta = lax.all_gather(mod_beta, "time", tiled=True).astype(jnp.float32)
        h = lax.all_gather(step_size, "time", tiled=True)
        top = jnp.max(jnp.abs(h)) * 16.0
        scale = jnp.where(top > 0, h / top, 0.0)
        hb = jnp.concatenate([jnp.broadcast_to(h[:, None], (T, C)), jnp.full((8, C), top)], 0)
        hs = jnp.broadcast_to(scale[:, None], (T, D))
        steps = rows // R
        full = lambda a: pl.BlockSpec(a.shape, lambda i, t: (0,) * a.ndim, pipeline_mode=pl.Buffered(1))
        args = (w_in, w_out, 0.5 + 0.5 * gamma, 0.5 * beta, hb, hs)
        out = pl.pallas_call(
            kernel,
            grid_spec=pltpu.PrefetchScalarGridSpec(
                num_scalar_prefetch=1, grid=(steps,),
                in_specs=[pl.BlockSpec((R, C), lambda i, t: (t[0] * steps + i, 0))] + [full(a) for a in args],
                out_specs=pl.BlockSpec((R, C), lambda i, t: (i, 0)),
                scratch_shapes=[pltpu.VMEM((R, D), jnp.float32), pltpu.VMEM((3 * R, C), jnp.float32),
                                pltpu.VMEM((3 * R, C), jnp.bfloat16), pltpu.VMEM((3 * R, D), jnp.bfloat16),
                                pltpu.VMEM((R, D), jnp.float32)],
            ),
            out_shape=jax.ShapeDtypeStruct((rows, C), jnp.float32),
            compiler_params=pltpu.CompilerParams(vmem_limit_bytes=60 * 2**20),
        )(me.astype(jnp.int32).reshape(1), x_init.reshape(-1, C), *args)
        return lax.all_gather(out, "time", tiled=True).reshape(x_init.shape)

    return jax.shard_map(local_run, mesh=mesh, in_specs=(P("data", None, None), P(None, None), P(None, None), P("time", None), P("time", None), P("time")), out_specs=P("data", None, None), check_vma=False)
```

```python
import functools

import jax
import jax.numpy as jnp
from jax import lax
from jax.experimental import pallas as pl
from jax.experimental.pallas import tpu as pltpu
from jax.sharding import PartitionSpec as P

R = 128
C = 768
D = 3072
T = 16
PER = 4
SPAN = 13
B = 256
NB = D // B
CB = C // B
PIECE = 64
K2 = 2.0 * 0.7978845608028654
K3 = 8.0 * 0.7978845608028654 * 0.044715
MESH = pl.DeviceIdType.MESH


def modulated_gelu(a, g, b):
    u = a * g + b
    t = jnp.tanh(u * ((u * u) * K3 + K2))
    return (u * t + u).astype(jnp.bfloat16)


def tile(w_ref, k, n):
    rows = slice(k * B, (k + 1) * B)
    return jnp.concatenate([w_ref[2 * n, rows], w_ref[2 * n + 1, rows]], axis=1)


def kernel(groups, base, chunks, x_ref, win_hbm, wout_hbm, mod_ref, h_ref, y_ref,
           win_ref, wout_ref, w_sem, mods, hs, xbuf, a0, lat, latb, hid, s_acc, ybase, ybuf, x_sem, y_sem):
    row0 = base + lax.axis_index("time") * (chunks * R)

    def x_copy(c):
        return pltpu.make_async_copy(x_ref.at[pl.ds(row0 + c * R, R)], xbuf.at[lax.rem(c, 2)], x_sem.at[lax.rem(c, 2)])

    def y_copy(c):
        return pltpu.make_async_copy(ybuf.at[lax.rem(c, 2)], y_ref.at[pl.ds(c * R, R)], y_sem.at[lax.rem(c, 2)])

    x_copy(0).start()
    loads = [pltpu.make_async_copy(w.at[:, pl.ds(i * 128, 128)], v.at[i], w_sem.at[at])
             for at, (w, v) in enumerate(((win_hbm, win_ref), (wout_hbm, wout_ref))) for i in range(v.shape[0])]
    for load in loads:
        load.start()
    half = 0.5 * mod_ref[...].astype(jnp.float32)
    mods[:, :, 0:D] = half[:, :, 0:D] + 0.5
    mods[:, :, D:2 * D] = half[:, :, D:2 * D]
    h = h_ref[...]
    mods[:, :, 2 * D:] = jnp.concatenate([h] * (C // 128), axis=2)
    top = jnp.max(jnp.max(jnp.abs(h), axis=0), axis=0, keepdims=True)
    top = jnp.concatenate([top] * (B // 128), axis=1)
    hs[0:groups] = (jnp.concatenate([h] * (B // 128), axis=2) / jnp.where(top > 0.0, top, 1.0)[None]) * 0.0625
    hs[groups] = jnp.broadcast_to(top, (PER, B))
    lat[...] = jnp.zeros_like(lat)
    latb[...] = jnp.zeros_like(latb)
    s_acc[...] = jnp.zeros_like(s_acc)
    for load in loads:
        load.wait()

    def body(acc1, acc2):
        count = [0, 0]

        def push(w, q):
            reg = count[q] % 2
            count[q] += 1
            pltpu.matmul_push_rhs(w, staging_register=reg, mxu_index=q)
            return reg

        def mm1_part(n, kt, q):
            reg = push(tile(win_ref, kt, n), q)
            for p in range(3):
                r = (q * 3 + p) * PIECE
                pltpu.matmul_acc_lhs(acc1[n % 2][q][p], latb[r:r + PIECE, kt * B:(kt + 1) * B],
                                     load_staged_rhs=reg if p == 0 else None)

        def mm2_part(n, m, q):
            reg = push(tile(wout_ref, n, m), q)
            for p in range(3):
                r = (q * 3 + p) * PIECE
                pltpu.matmul_acc_lhs(acc2[m][q][p], hid[r:r + PIECE, n * B:(n + 1) * B],
                                     load_staged_rhs=reg if p == 0 else None)

        def mm2(n):
            for m in range(CB):
                for q in range(2):
                    mm2_part(n, m, q)

        def row(ref, j, cols):
            return ref[pl.ds(lax.div(j, PER), 1), pl.ds(lax.rem(j, PER), 1), cols][0]

        def mod_rows(j, n):
            return row(mods, j, pl.ds(n * B, B)), row(mods, j, pl.ds(D + n * B, B))

        def first_part(n, half, js):
            cs = slice(n * B, (n + 1) * B)
            r = half * PIECE
            hid[r:r + PIECE, cs] = modulated_gelu(a0[r:r + PIECE, cs], *mod_rows(js[0], n))

        def act_part(n, i, js):
            cs = slice(n * B, (n + 1) * B)
            s = 1 + i // 2
            a = pltpu.matmul_pop(acc1[n % 2][i // 3][i % 3])
            v = modulated_gelu(a, *mod_rows(js[s], n))
            r = (i % 2) * PIECE
            if s < 3:
                hid[s * R + r:s * R + r + PIECE, cs] = v
            else:
                s_acc[r:r + PIECE, cs] += v.astype(jnp.float32) * row(hs, js[3], slice(0, B))

        def step(k, ramp):
            js = [jnp.int32(k + SPAN if ramp and k < s else k) for s in range(4)]
            for n in range(NB + LAG):
                for half in range(2):
                    vpu = []
                    if half == 0 and 1 <= n <= NB:
                        vpu = [functools.partial(act_part, n - 1, i, js) for i in (3, 4, 5)]
                    if half == 1 and n < NB:
                        vpu = [functools.partial(act_part, n, i, js) for i in range(3)]
                    if n < NB:
                        vpu = vpu[:2] + [functools.partial(first_part, n, half, js)] + vpu[2:]
                    done = 0
                    for at in range(CB):
                        for q in range(2):
                            if half == q:
                                if n < NB:
                                    mm1_part(n, at, q)
                            elif n >= LAG:
                                mm2_part(n - LAG, at, q)
                        upto = len(vpu) * (at + 1) // CB
                        for v in vpu[done:upto]:
                            v()
                        done = upto
            for m in range(CB):
                ms = slice(m * B, (m + 1) * B)
                for i in (4, 5, 2, 3, 0, 1):
                    sweep, r = i // 2, R + i * PIECE
                    base = r - R if ramp and k == sweep else r
                    new = lat[base:base + PIECE, ms] + pltpu.matmul_pop(acc2[m][i // 3][i % 3]) * row(mods, js[sweep], pl.ds(2 * D + m * B, B))
                    lat[r:r + PIECE, ms] = new
                    latb[r - R:r - R + PIECE, ms] = new.astype(jnp.bfloat16)

        def enter(c):
            x_copy(c).wait()
            @pl.when(c + 1 < chunks)
            def _():
                x_copy(c + 1).start()
            x0 = xbuf[lax.rem(c, 2)]
            lat[0:R] = x0
            hid[0:R, 0:C] = x0.astype(jnp.bfloat16)
            for n in range(NB):
                q = n % 2
                for kt in range(CB):
                    reg = push(tile(win_ref, kt, n), q)
                    for p in range(2):
                        pltpu.matmul_acc_lhs(acc1[n // 2 % 2][q][p], hid[p * PIECE:(p + 1) * PIECE, kt * B:(kt + 1) * B],
                                             load_staged_rhs=reg if p == 0 else None)
                for p in range(2):
                    a0[p * PIECE:(p + 1) * PIECE, n * B:(n + 1) * B] = pltpu.matmul_pop(acc1[n // 2 % 2][q][p])

        def leave(c):
            for n in range(NB):
                cs = slice(n * B, (n + 1) * B)
                sv = s_acc[:, cs]
                top = sv.astype(jnp.bfloat16)
                rest = sv - top.astype(jnp.float32)
                mid = rest.astype(jnp.bfloat16)
                hid[0:R, cs] = top
                hid[R:2 * R, cs] = mid
                hid[2 * R:3 * R, cs] = (rest - mid.astype(jnp.float32)).astype(jnp.bfloat16)
                mm2(n)
            slot = lax.rem(c, 2)
            @pl.when(c >= 2)
            def _():
                y_copy(c - 2).wait()
            for m in range(CB):
                ms = slice(m * B, (m + 1) * B)
                d = [pltpu.matmul_pop(acc2[m][i // 3][i % 3]) for i in range(6)]
                for half in range(2):
                    rs = slice(half * PIECE, (half + 1) * PIECE)
                    ybuf[slot, rs, ms] = ybase[rs, ms] + ((d[half] + (d[2 + half] + d[4 + half])) * 16.0) * hs[groups, 0:1, 0:B]
            y_copy(c).start()

        enter(jnp.int32(0))

        @pl.loop(0, chunks + 1)
        def _(c):
            for k in range(3):
                step(k, True)

            @pl.when(c > 0)
            def _():
                leave(c - 1)

            @pl.when(c < chunks)
            def _():
                ybase[...] = lat[3 * R:4 * R]
                s_acc[...] = jnp.zeros_like(s_acc)

                @pl.loop(0, (SPAN - 3) // UNROLL)
                def _(i):
                    for u in range(UNROLL):
                        step(3 + i * UNROLL + u, False)

            @pl.when(c + 1 < chunks)
            def _():
                enter(c + 1)

        for c in (chunks - 2, chunks - 1):
            y_copy(jnp.int32(c)).wait()

    acc = lambda q: pltpu.ACC(q)((PIECE, B), jnp.float32)
    pl.run_scoped(body, tuple(tuple(tuple(acc(q) for _ in range(3)) for q in range(2)) for _ in range(2)),
                  tuple(tuple(tuple(acc(q) for _ in range(3)) for q in range(2)) for _ in range(CB)))


LAG = 3
UNROLL = 1


def sampler(groups, base, chunks, x, *args):
    hbm = pl.BlockSpec(memory_space=pl.ANY)
    vmem = pl.BlockSpec(memory_space=pltpu.VMEM)
    dma = pltpu.SemaphoreType.DMA
    return pl.pallas_call(
        functools.partial(kernel, groups, base, chunks),
        out_shape=jax.ShapeDtypeStruct((chunks * R, C), jnp.float32),
        in_specs=[hbm] * 3 + [vmem] * 2, out_specs=hbm,
        scratch_shapes=[
            pltpu.VMEM((D // 128, C, 128), jnp.bfloat16), pltpu.VMEM((C // 128, D, 128), jnp.bfloat16), dma((2,)),
            pltpu.VMEM((groups, PER, 2 * D + C), jnp.float32), pltpu.VMEM((groups + 1, PER, B), jnp.float32),
            pltpu.VMEM((2, R, C), jnp.float32), pltpu.VMEM((R, D), jnp.float32), pltpu.VMEM((4 * R, C), jnp.float32),
            pltpu.VMEM((3 * R, C), jnp.bfloat16), pltpu.VMEM((3 * R, D), jnp.bfloat16), pltpu.VMEM((R, D), jnp.float32),
            pltpu.VMEM((R, C), jnp.float32), pltpu.VMEM((2, R, C), jnp.float32),
            dma((2,)), dma((2,)),
        ],
        compiler_params=pltpu.CompilerParams(vmem_limit_bytes=60 * 2**20),
        cost_estimate=pl.CostEstimate(flops=chunks * R * C * D * 2 * 90, bytes_accessed=20 * 2**20, transcendentals=0),
    )(x, *args)


def gather_kernel(groups, mod_ref, h_ref, mods, hs, own_sem, send_sem, recv_sem):
    me = lax.axis_index("time")
    barrier = pltpu.get_barrier_semaphore()
    for d in range(1, groups):
        pl.semaphore_signal(barrier, inc=1, device_id={"time": lax.rem(me + d, groups)}, device_id_type=MESH)
    own = [pltpu.make_async_copy(src, dst.at[me], own_sem.at[i]) for i, (src, dst) in enumerate(((mod_ref, mods), (h_ref, hs)))]
    for copy in own:
        copy.start()
    pl.semaphore_wait(barrier, groups - 1)
    sends = [pltpu.make_async_remote_copy(
        src_ref=src, dst_ref=dst.at[me], send_sem=send_sem.at[i, d - 1], recv_sem=recv_sem.at[i, d - 1],
        device_id={"time": lax.rem(me + d, groups)}, device_id_type=MESH)
        for d in range(1, groups) for i, (src, dst) in enumerate(((mod_ref, mods), (h_ref, hs)))]
    for send in sends:
        send.start()
    for send in sends:
        send.wait()
    for copy in own:
        copy.wait()


def gather(groups, mod, h):
    vmem = pl.BlockSpec(memory_space=pltpu.VMEM)
    dma = pltpu.SemaphoreType.DMA
    return pl.pallas_call(
        functools.partial(gather_kernel, groups),
        out_shape=[jax.ShapeDtypeStruct((groups,) + a.shape, a.dtype) for a in (mod, h)],
        in_specs=[vmem] * 2, out_specs=[vmem] * 2,
        scratch_shapes=[dma((2,)), dma((2, groups - 1)), dma((2, groups - 1))],
        compiler_params=pltpu.CompilerParams(collective_id=0, has_side_effects=True),
    )(mod, h)


def place_kernel(base, skip, *refs):
    blocks, (y_ref, buf, load_sem, store_sem) = refs[skip:-4], refs[-4:]
    me = lax.axis_index("time")
    rows = buf.shape[1]
    loads = [pltpu.make_async_copy(block, buf.at[d], load_sem.at[d]) for d, block in enumerate(blocks)]
    stores = [pltpu.make_async_copy(buf.at[d], y_ref.at[pl.ds(base + (me ^ d) * rows, rows)], store_sem.at[d]) for d in range(len(blocks))]
    for load in loads:
        load.start()
    for load, store in zip(loads, stores):
        load.wait()
        store.start()
    for store in stores:
        store.wait()


def place(base, total, blocks, y=None):
    hbm = pl.BlockSpec(memory_space=pl.ANY)
    dma = pltpu.SemaphoreType.DMA
    held = [] if y is None else [y]
    return pl.pallas_call(
        functools.partial(place_kernel, base, len(held)),
        out_shape=jax.ShapeDtypeStruct((total, C), jnp.float32),
        in_specs=[hbm] * (len(held) + len(blocks)), out_specs=hbm,
        scratch_shapes=[pltpu.VMEM((len(blocks),) + blocks[0].shape, jnp.float32), dma((len(blocks),)), dma((len(blocks),))],
        input_output_aliases={0: 0} if held else {},
        cost_estimate=pl.CostEstimate(flops=0, bytes_accessed=2 * 4 * len(blocks) * blocks[0].size, transcendentals=0),
    )(*held, *blocks)


LAST = 2


def solution(mesh):
    groups = mesh.shape["time"]
    swap = lambda a, d: lax.ppermute(a, "time", [(i, i ^ d) for i in range(groups)])

    def local_run(x_init, w_in, w_out, mod_gamma, mod_beta, step_size):
        x = x_init.reshape(-1, C)
        total = x.shape[0]
        args = gather(groups, jnp.concatenate([mod_gamma, mod_beta], axis=1), jnp.broadcast_to(step_size[:, None], (PER, 128)))
        chunks = total // (groups * R)
        split = (chunks - LAST) * R * groups
        early = sampler(groups, 0, chunks - LAST, x, w_in, w_out, *args)
        others = [swap(early, d) for d in range(1, groups)]
        late = sampler(groups, split, LAST, x, w_in, w_out, *args)
        across = swap(late, 2)
        y = place(0, total, [early] + others)
        y = place(split, total, [late, swap(late, 1), across, swap(across, 1)], y)
        return y.reshape(x_init.shape)

    return jax.shard_map(local_run, mesh=mesh, in_specs=(P("data", None, None), P(None, None), P(None, None), P("time", None), P("time", None), P("time")), out_specs=P("data", None, None), check_vma=False)
```

```python
import functools

import jax
import jax.numpy as jnp
from jax import lax
from jax.experimental import pallas as pl
from jax.experimental.pallas import tpu as pltpu
from jax.sharding import PartitionSpec as P

R = 128
C = 768
D = 3072
T = 16
PER = 4
SPAN = 13
B = 256
NB = D // B
CB = C // B
PIECE = 64
K2 = 2.0 * 0.7978845608028654
K3 = 8.0 * 0.7978845608028654 * 0.044715
MESH = pl.DeviceIdType.MESH


def modulated_gelu(a, g, b):
    u = a * g + b
    t = jnp.tanh(u * ((u * u) * K3 + K2))
    return (u * t + u).astype(jnp.bfloat16)


def tile(w_ref, k, n):
    rows = slice(k * B, (k + 1) * B)
    return jnp.concatenate([w_ref[2 * n, rows], w_ref[2 * n + 1, rows]], axis=1)


def kernel(groups, base, chunks, x_ref, win_hbm, wout_hbm, gamma_ref, beta_ref, h_ref, y_ref,
           win_ref, wout_ref, w_sem, mods, hs, xbuf, a0, lat, latb, hid, s_acc, ybase, ybuf, x_sem, y_sem):
    row0 = base + lax.axis_index("time") * (chunks * R)

    def x_copy(c):
        return pltpu.make_async_copy(x_ref.at[pl.ds(row0 + c * R, R)], xbuf.at[lax.rem(c, 2)], x_sem.at[lax.rem(c, 2)])

    def y_copy(c):
        return pltpu.make_async_copy(ybuf.at[lax.rem(c, 2)], y_ref.at[pl.ds(c * R, R)], y_sem.at[lax.rem(c, 2)])

    x_copy(0).start()
    loads = [pltpu.make_async_copy(w.at[:, pl.ds(i * 128, 128)], v.at[i], w_sem.at[at])
             for at, (w, v) in enumerate(((win_hbm, win_ref), (wout_hbm, wout_ref))) for i in range(v.shape[0])]
    for load in loads:
        load.start()
    mods[:, :, 0:D] = 0.5 * gamma_ref[...].astype(jnp.float32) + 0.5
    mods[:, :, D:2 * D] = 0.5 * beta_ref[...].astype(jnp.float32)
    h = h_ref[...]
    mods[:, :, 2 * D:] = jnp.concatenate([h] * (C // 128), axis=2)
    top = jnp.max(jnp.max(jnp.abs(h), axis=0), axis=0, keepdims=True)
    top = jnp.concatenate([top] * (B // 128), axis=1)
    hs[0:groups] = (jnp.concatenate([h] * (B // 128), axis=2) / jnp.where(top > 0.0, top, 1.0)[None]) * 0.0625
    hs[groups] = jnp.broadcast_to(top, (PER, B))
    lat[...] = jnp.zeros_like(lat)
    latb[...] = jnp.zeros_like(latb)
    s_acc[...] = jnp.zeros_like(s_acc)
    for load in loads[:win_ref.shape[0]]:
        load.wait()

    def body(acc1, acc2):
        count = [0, 0]

        def push(w, q):
            reg = count[q] % 2
            count[q] += 1
            pltpu.matmul_push_rhs(w, staging_register=reg, mxu_index=q)
            return reg

        def mm1_part(n, kt, q):
            reg = push(tile(win_ref, kt, n), q)
            for p in range(3):
                r = (q * 3 + p) * PIECE
                pltpu.matmul_acc_lhs(acc1[n % 2][q][p], latb[r:r + PIECE, kt * B:(kt + 1) * B],
                                     load_staged_rhs=reg if p == 0 else None)

        def mm2_part(n, m, q):
            reg = push(tile(wout_ref, n, m), q)
            for p in range(3):
                r = (q * 3 + p) * PIECE
                pltpu.matmul_acc_lhs(acc2[m][q][p], hid[r:r + PIECE, n * B:(n + 1) * B],
                                     load_staged_rhs=reg if p == 0 else None)

        def mm2(n):
            for m in range(CB):
                for q in range(2):
                    mm2_part(n, m, q)

        def row(ref, j, cols):
            return ref[pl.ds(lax.div(j, PER), 1), pl.ds(lax.rem(j, PER), 1), cols][0]

        def mod_rows(j, n):
            return row(mods, j, pl.ds(n * B, B)), row(mods, j, pl.ds(D + n * B, B))

        def first_part(n, half, js):
            cs = slice(n * B, (n + 1) * B)
            r = half * PIECE
            hid[r:r + PIECE, cs] = modulated_gelu(a0[r:r + PIECE, cs], *mod_rows(js[0], n))

        def act_part(n, i, js):
            cs = slice(n * B, (n + 1) * B)
            s = 1 + i // 2
            a = pltpu.matmul_pop(acc1[n % 2][i // 3][i % 3])
            v = modulated_gelu(a, *mod_rows(js[s], n))
            r = (i % 2) * PIECE
            if s < 3:
                hid[s * R + r:s * R + r + PIECE, cs] = v
            else:
                s_acc[r:r + PIECE, cs] += v.astype(jnp.float32) * row(hs, js[3], slice(0, B))

        def step(js):
            for n in range(NB + LAG):
                for half in range(2):
                    vpu = []
                    if half == 0 and 1 <= n <= NB:
                        vpu = [functools.partial(act_part, n - 1, i, js) for i in (3, 4, 5)]
                    if half == 1 and n < NB:
                        vpu = [functools.partial(act_part, n, i, js) for i in range(3)]
                    if n < NB:
                        vpu = vpu[:2] + [functools.partial(first_part, n, half, js)] + vpu[2:]
                    done = 0
                    for at in range(CB):
                        for q in range(2):
                            if half == q:
                                if n < NB:
                                    mm1_part(n, at, q)
                            elif n >= LAG:
                                mm2_part(n - LAG, at, q)
                        upto = len(vpu) * (at + 1) // CB
                        for v in vpu[done:upto]:
                            v()
                        done = upto
            for m in range(CB):
                ms = slice(m * B, (m + 1) * B)
                for i in (4, 5, 2, 3, 0, 1):
                    sweep, r = i // 2, R + i * PIECE
                    new = lat[r:r + PIECE, ms] + pltpu.matmul_pop(acc2[m][i // 3][i % 3]) * row(mods, js[sweep], pl.ds(2 * D + m * B, B))
                    lat[r:r + PIECE, ms] = new
                    latb[r - R:r - R + PIECE, ms] = new.astype(jnp.bfloat16)

        def enter(c):
            x_copy(c).wait()
            @pl.when(c + 1 < chunks)
            def _():
                x_copy(c + 1).start()
            x0 = xbuf[lax.rem(c, 2)]
            lat[0:R] = x0
            hid[0:R, 0:C] = x0.astype(jnp.bfloat16)
            for n in range(NB):
                q = n % 2
                for kt in range(CB):
                    reg = push(tile(win_ref, kt, n), q)
                    for p in range(2):
                        pltpu.matmul_acc_lhs(acc1[n // 2 % 2][q][p], hid[p * PIECE:(p + 1) * PIECE, kt * B:(kt + 1) * B],
                                             load_staged_rhs=reg if p == 0 else None)
                for p in range(2):
                    a0[p * PIECE:(p + 1) * PIECE, n * B:(n + 1) * B] = pltpu.matmul_pop(acc1[n // 2 % 2][q][p])

        def leave(c):
            for n in range(NB):
                cs = slice(n * B, (n + 1) * B)
                sv = s_acc[:, cs]
                top = sv.astype(jnp.bfloat16)
                rest = sv - top.astype(jnp.float32)
                mid = rest.astype(jnp.bfloat16)
                hid[0:R, cs] = top
                hid[R:2 * R, cs] = mid
                hid[2 * R:3 * R, cs] = (rest - mid.astype(jnp.float32)).astype(jnp.bfloat16)
                mm2(n)
            slot = lax.rem(c, 2)
            @pl.when(c >= 2)
            def _():
                y_copy(c - 2).wait()
            for m in range(CB):
                ms = slice(m * B, (m + 1) * B)
                d = [pltpu.matmul_pop(acc2[m][i // 3][i % 3]) for i in range(6)]
                for half in range(2):
                    rs = slice(half * PIECE, (half + 1) * PIECE)
                    ybuf[slot, rs, ms] = ybase[rs, ms] + ((d[half] + (d[2 + half] + d[4 + half])) * 16.0) * hs[groups, 0:1, 0:B]
            y_copy(c).start()

        enter(jnp.int32(0))
        for load in loads[win_ref.shape[0]:]:
            load.wait()

        @pl.loop(0, chunks + 1)
        def _(c):
            @pl.loop(0, jnp.where(c < chunks, SPAN, 3))
            def _(k):
                for s in range(3):
                    @pl.when(k == s)
                    def _():
                        lat[(s + 1) * R:(s + 2) * R] = lat[s * R:(s + 1) * R]

                @pl.when(k == 3)
                def _():
                    ybase[...] = lat[3 * R:4 * R]
                    s_acc[...] = jnp.zeros_like(s_acc)

                step([jnp.where(k >= s, k, k + SPAN) for s in range(4)])

                @pl.when((k == 2) & (c > 0))
                def _():
                    leave(c - 1)

            @pl.when(c + 1 < chunks)
            def _():
                enter(c + 1)

        for c in range(max(chunks - 2, 0), chunks):
            y_copy(jnp.int32(c)).wait()

    acc = lambda q: pltpu.ACC(q)((PIECE, B), jnp.float32)
    pl.run_scoped(body, tuple(tuple(tuple(acc(q) for _ in range(3)) for q in range(2)) for _ in range(2)),
                  tuple(tuple(tuple(acc(q) for _ in range(3)) for q in range(2)) for _ in range(CB)))


LAG = 3


def sampler(groups, base, chunks, x, *args):
    hbm = pl.BlockSpec(memory_space=pl.ANY)
    vmem = pl.BlockSpec(memory_space=pltpu.VMEM)
    dma = pltpu.SemaphoreType.DMA
    return pl.pallas_call(
        functools.partial(kernel, groups, base, chunks),
        out_shape=jax.ShapeDtypeStruct((chunks * R, C), jnp.float32),
        in_specs=[hbm] * 3 + [vmem] * 3, out_specs=hbm,
        scratch_shapes=[
            pltpu.VMEM((D // 128, C, 128), jnp.bfloat16), pltpu.VMEM((C // 128, D, 128), jnp.bfloat16), dma((2,)),
            pltpu.VMEM((groups, PER, 2 * D + C), jnp.float32), pltpu.VMEM((groups + 1, PER, B), jnp.float32),
            pltpu.VMEM((2, R, C), jnp.float32), pltpu.VMEM((R, D), jnp.float32), pltpu.VMEM((4 * R, C), jnp.float32),
            pltpu.VMEM((3 * R, C), jnp.bfloat16), pltpu.VMEM((3 * R, D), jnp.bfloat16), pltpu.VMEM((R, D), jnp.float32),
            pltpu.VMEM((R, C), jnp.float32), pltpu.VMEM((2, R, C), jnp.float32),
            dma((2,)), dma((2,)),
        ],
        compiler_params=pltpu.CompilerParams(vmem_limit_bytes=60 * 2**20),
        cost_estimate=pl.CostEstimate(flops=chunks * R * C * D * 2 * 90, bytes_accessed=20 * 2**20, transcendentals=0),
    )(x, *args)


def gather_kernel(groups, gamma_ref, beta_ref, h_ref, gammas, betas, hs, own_sem, send_sem, recv_sem):
    me = lax.axis_index("time")
    barrier = pltpu.get_barrier_semaphore()
    for d in range(1, groups):
        pl.semaphore_signal(barrier, inc=1, device_id={"time": lax.rem(me + d, groups)}, device_id_type=MESH)
    own = [pltpu.make_async_copy(src, dst.at[me], own_sem.at[i]) for i, (src, dst) in enumerate(((gamma_ref, gammas), (beta_ref, betas), (h_ref, hs)))]
    for copy in own:
        copy.start()
    pl.semaphore_wait(barrier, groups - 1)
    sends = [pltpu.make_async_remote_copy(
        src_ref=src, dst_ref=dst.at[me], send_sem=send_sem.at[i, d - 1], recv_sem=recv_sem.at[i, d - 1],
        device_id={"time": lax.rem(me + d, groups)}, device_id_type=MESH)
        for d in range(1, groups) for i, (src, dst) in enumerate(((gamma_ref, gammas), (beta_ref, betas), (h_ref, hs)))]
    for send in sends:
        send.start()
    for send in sends:
        send.wait()
    for copy in own:
        copy.wait()


def gather(groups, *arrays):
    vmem = pl.BlockSpec(memory_space=pltpu.VMEM)
    dma = pltpu.SemaphoreType.DMA
    return pl.pallas_call(
        functools.partial(gather_kernel, groups),
        out_shape=[jax.ShapeDtypeStruct((groups,) + a.shape, a.dtype) for a in arrays],
        in_specs=[vmem] * 3, out_specs=[vmem] * 3,
        scratch_shapes=[dma((3,)), dma((3, groups - 1)), dma((3, groups - 1))],
        compiler_params=pltpu.CompilerParams(collective_id=0, has_side_effects=True),
    )(*arrays)


def place_kernel(base, skip, *refs):
    blocks, (y_ref, buf, load_sem, store_sem) = refs[skip:-4], refs[-4:]
    me = lax.axis_index("time")
    rows = buf.shape[1]
    loads = [pltpu.make_async_copy(block, buf.at[d], load_sem.at[d]) for d, block in enumerate(blocks)]
    stores = [pltpu.make_async_copy(buf.at[d], y_ref.at[pl.ds(base + (me ^ d) * rows, rows)], store_sem.at[d]) for d in range(len(blocks))]
    for load in loads:
        load.start()
    for load, store in zip(loads, stores):
        load.wait()
        store.start()
    for store in stores:
        store.wait()


def place(base, total, blocks, y=None):
    hbm = pl.BlockSpec(memory_space=pl.ANY)
    dma = pltpu.SemaphoreType.DMA
    held = [] if y is None else [y]
    return pl.pallas_call(
        functools.partial(place_kernel, base, len(held)),
        out_shape=jax.ShapeDtypeStruct((total, C), jnp.float32),
        in_specs=[hbm] * (len(held) + len(blocks)), out_specs=hbm,
        scratch_shapes=[pltpu.VMEM((len(blocks),) + blocks[0].shape, jnp.float32), dma((len(blocks),)), dma((len(blocks),))],
        input_output_aliases={0: 0} if held else {},
        cost_estimate=pl.CostEstimate(flops=0, bytes_accessed=2 * 4 * len(blocks) * blocks[0].size, transcendentals=0),
    )(*held, *blocks)


LAST = 1


def solution(mesh):
    groups = mesh.shape["time"]
    swap = lambda a, d: lax.ppermute(a, "time", [(i, i ^ d) for i in range(groups)])

    def local_run(x_init, w_in, w_out, mod_gamma, mod_beta, step_size):
        x = x_init.reshape(-1, C)
        total = x.shape[0]
        args = gather(groups, mod_gamma, mod_beta, jnp.broadcast_to(step_size[:, None], (PER, 128)))
        chunks = total // (groups * R)
        split = (chunks - LAST) * R * groups
        early = sampler(groups, 0, chunks - LAST, x, w_in, w_out, *args)
        early_across = swap(early, 2)
        late = sampler(groups, split, LAST, x, w_in, w_out, *args)
        early_across, late = lax.optimization_barrier((early_across, late))
        across = swap(late, 2)
        y = place(0, total, [early, swap(early, 1), early_across, swap(early_across, 1)])
        across, y = lax.optimization_barrier((across, y))
        y = place(split, total, [late, swap(late, 1), across, swap(across, 1)], y)
        return y.reshape(x_init.shape)

    return jax.shard_map(local_run, mesh=mesh, in_specs=(P("data", None, None), P(None, None), P(None, None), P("time", None), P("time", None), P("time")), out_specs=P("data", None, None), check_vma=False)
```
